32 devices in a mesh: tile: 8 (over y, x, core), head: 4 (over z).
Axes of the slice: x: 2, y: 2, z: 4, core: 2. Of those that a mesh axis runs over, the one named last changes fastest.
Arguments:
- latent: bfloat16 [16, 512, 512], P('tile', 'head'), may hold values from -6 to 6
- norm1_gain: float32 [512], replicated, may hold values from 0.25 to 1.75
- norm1_shift: float32 [512], replicated, may hold values from -1.75 to 1.75
- conv1_weight: bfloat16 [3, 3, 512, 512], replicated, may hold values from -0.09375 to 0.09375
- conv1_bias: float32 [512], replicated, may hold values from -1.75 to 1.75
- norm2_gain: float32 [512], replicated, may hold values from 0.25 to 1.75
- norm2_shift: float32 [512], replicated, may hold values from -1.75 to 1.75
- conv2_weight: bfloat16 [3, 3, 512, 512], replicated, may hold values from -0.09375 to 0.09375
- conv2_bias: float32 [512], replicated, may hold values from -1.75 to 1.75
- norm3_gain: float32 [512], replicated, may hold values from 0.25 to 1.75
- norm3_shift: float32 [512], replicated, may hold values from -1.75 to 1.75
- query_weight: bfloat16 [512, 512], replicated, may hold values from -2 to 2
- query_bias: float32 [512], replicated, may hold values from -3 to 3
- key_weight: bfloat16 [512, 512], replicated, may hold values from -2 to 2
- value_weight: bfloat16 [512, 512], replicated, may hold values from -0.25 to 0.25
- value_bias: float32 [512], replicated, may hold values from -3 to 3
- out_weight: bfloat16 [512, 512], replicated, may hold values from -0.5 to 0.5
- out_bias: float32 [512], replicated, may hold values from -1.75 to 1.75
Outputs:
- block_out: bfloat16 [16, 512, 512], P('tile', 'head')
The draws below stay inside these ranges and needn't reach their ends.
All inputs are finite; a program needn't handle non-finite values.
Results may differ from the reference program's by a relative error of at most 0.01615.
Values may be sent and summed in bfloat16 or wider, within the bound.
A program may use at most 128 MiB of HBM per device.

```python
import jax
import jax.numpy as jnp
from jax import lax

C = 512
GROUPS = 32
W = 512
H = 16


def base_projection(key, salt):
    entries = jax.random.normal(jax.random.fold_in(key, salt), (C, C), jnp.float32)
    return jnp.clip(entries, -4.0, 4.0) * (1.0 / jnp.sqrt(jnp.float32(C // 4)))


def draw_query_weight(key, part):
    weight = base_projection(key, 311)
    return weight.astype(jnp.bfloat16)


def draw_key_weight(key, part):
    weight = base_projection(key, 523)
    return weight.astype(jnp.bfloat16)


def smooth_field(key):
    freq_rows = jax.random.randint(jax.random.fold_in(key, 7101), (4,), 1, 4).astype(jnp.float32)
    freq_cols = jax.random.randint(jax.random.fold_in(key, 7102), (4,), 0, 4).astype(jnp.float32)
    phases = jax.random.uniform(jax.random.fold_in(key, 7103), (4,), jnp.float32, -jnp.pi, jnp.pi)
    amplitudes = jax.random.uniform(jax.random.fold_in(key, 7104), (4,), jnp.float32, 0.5, 0.9)
    row_pos = jnp.arange(H, dtype=jnp.float32) / jnp.float32(H)
    col_pos = jnp.arange(W, dtype=jnp.float32) / jnp.float32(W)
    phase_grid = 2.0 * jnp.pi * (freq_rows[:, None, None] * row_pos[None, :, None] + freq_cols[:, None, None] * col_pos[None, None, :]) + phases[:, None, None]
    return jnp.sum(amplitudes[:, None, None] * jnp.cos(phase_grid), axis=0) + 0.4


def draw_latent(key, part):
    field = smooth_field(key)
    loading = jax.random.normal(jax.random.fold_in(key, 7105), (C,), jnp.float32)
    noise = 0.7 * jax.random.normal(jax.random.fold_in(key, 7106), (H, W, C), jnp.float32)
    values = noise + field[:, :, None] * loading[None, None, :]
    return jnp.clip(values, -6.0, 6.0).astype(jnp.bfloat16)


def gaussian(key, dims, scale, most, kind=jnp.bfloat16):
    return jnp.clip(scale * jax.random.normal(key, dims, jnp.float32), -most, most).astype(kind)


def setup_inputs(seed: int = 0) -> dict:
    arg_keys = jax.random.split(jax.random.key(seed), 19)
    latent = draw_latent(jax.random.fold_in(arg_keys[18], 71), 0)
    norm1_gain = jnp.clip(1.0 + 0.15 * jax.random.normal(arg_keys[1], (C,), jnp.float32), 0.25, 1.75)
    norm1_shift = gaussian(arg_keys[2], (C,), 0.3, 1.75, jnp.float32)
    conv1_weight = gaussian(arg_keys[3], (3, 3, C, C), (9 * C) ** -0.5, 0.09375)
    conv1_bias = gaussian(arg_keys[4], (C,), 0.3, 1.75, jnp.float32)
    norm2_gain = jnp.clip(1.0 + 0.15 * jax.random.normal(arg_keys[5], (C,), jnp.float32), 0.25, 1.75)
    norm2_shift = gaussian(arg_keys[6], (C,), 0.3, 1.75, jnp.float32)
    conv2_weight = gaussian(arg_keys[7], (3, 3, C, C), (9 * C) ** -0.5, 0.09375)
    conv2_bias = gaussian(arg_keys[8], (C,), 0.3, 1.75, jnp.float32)
    norm3_gain = jnp.clip(1.0 + 0.15 * jax.random.normal(arg_keys[9], (C,), jnp.float32), 0.25, 1.75)
    norm3_shift = gaussian(arg_keys[10], (C,), 0.3, 1.75, jnp.float32)
    query_weight = draw_query_weight(jax.random.fold_in(arg_keys[18], 71), 0)
    query_bias = gaussian(arg_keys[12], (C,), 0.5, 3.0, jnp.float32)
    key_weight = draw_key_weight(jax.random.fold_in(arg_keys[18], 71), 0)
    value_weight = gaussian(arg_keys[14], (C, C), C ** -0.5, 0.25)
    value_bias = gaussian(arg_keys[15], (C,), 0.5, 3.0, jnp.float32)
    out_weight = gaussian(arg_keys[16], (C, C), (C // 4) ** -0.5, 0.5)
    out_bias = gaussian(arg_keys[17], (C,), 0.3, 1.75, jnp.float32)
    return dict(latent=latent, norm1_gain=norm1_gain, norm1_shift=norm1_shift, conv1_weight=conv1_weight, conv1_bias=conv1_bias, norm2_gain=norm2_gain, norm2_shift=norm2_shift, conv2_weight=conv2_weight, conv2_bias=conv2_bias, norm3_gain=norm3_gain, norm3_shift=norm3_shift, query_weight=query_weight, query_bias=query_bias, key_weight=key_weight, value_weight=value_weight, value_bias=value_bias, out_weight=out_weight, out_bias=out_bias)


def group_norm(values, gain, shift):
    grouped = values.reshape(-1, GROUPS, C // GROUPS)
    mean = lax.optimization_barrier(jnp.mean(grouped, axis=(0, 2)))
    deviation = grouped - mean[None, :, None]
    variance = lax.optimization_barrier(jnp.mean(deviation * deviation, axis=(0, 2)))
    normalized = deviation * lax.rsqrt(variance + 1e-06)[None, :, None]
    return normalized.reshape(values.shape) * gain + shift

def conv_three(act, weight, bias):
    result = lax.conv_general_dilated(act[None], weight, (1, 1), ((1, 1), (1, 1)), dimension_numbers=('NHWC', 'HWIO', 'NHWC'), preferred_element_type=jnp.float32)[0]
    return result + bias

def reference(latent, norm1_gain, norm1_shift, conv1_weight, conv1_bias, norm2_gain, norm2_shift, conv2_weight, conv2_bias, norm3_gain, norm3_shift, query_weight, query_bias, key_weight, value_weight, value_bias, out_weight, out_bias):
    latent32 = latent.astype(jnp.float32)
    act1 = jax.nn.silu(group_norm(latent32, norm1_gain, norm1_shift)).astype(jnp.bfloat16)
    hidden = conv_three(act1, conv1_weight, conv1_bias)
    act2 = jax.nn.silu(group_norm(hidden, norm2_gain, norm2_shift)).astype(jnp.bfloat16)
    resid = (latent32 + conv_three(act2, conv2_weight, conv2_bias)).astype(jnp.bfloat16)
    flat_res = resid.reshape(-1, C)
    normed = group_norm(flat_res.astype(jnp.float32), norm3_gain, norm3_shift).astype(jnp.bfloat16)
    queries = (jnp.dot(normed, query_weight, preferred_element_type=jnp.float32) + query_bias).astype(jnp.bfloat16)
    keys = jnp.dot(normed, key_weight, preferred_element_type=jnp.float32).astype(jnp.bfloat16)
    values = (jnp.dot(normed, value_weight, preferred_element_type=jnp.float32) + value_bias).astype(jnp.bfloat16)
    total_rows = queries.shape[0]
    block_rows = 1024 if total_rows % 1024 == 0 else total_rows
    softmax_scale = 1.0 / C ** 0.5

    def attend(query_block):
        scores = jnp.dot(query_block, keys.T, preferred_element_type=jnp.float32) * softmax_scale
        top = lax.optimization_barrier(jnp.max(scores, axis=1, keepdims=True))
        expo = jnp.exp(scores - top)
        row_sum = lax.optimization_barrier(jnp.sum(expo, axis=1, keepdims=True))
        weighted = jnp.dot(expo.astype(jnp.bfloat16), values, preferred_element_type=jnp.float32)
        return (weighted / row_sum).astype(jnp.bfloat16)
    attended = lax.map(attend, queries.reshape(total_rows // block_rows, block_rows, C)).reshape(total_rows, C)
    mixed = flat_res.astype(jnp.float32) + jnp.dot(attended, out_weight, preferred_element_type=jnp.float32) + out_bias
    return mixed.astype(jnp.bfloat16).reshape(latent.shape)
```

```python
import functools

import jax
import jax.numpy as jnp
from jax import lax
from jax.experimental import pallas as pl
from jax.experimental.pallas import tpu as pltpu
from jax.sharding import PartitionSpec as P

C = 512
GROUPS = 32
WIDTH = C // GROUPS
EPS = 1e-06
MESH = pl.DeviceIdType.MESH
VMEM = pl.BlockSpec(memory_space=pltpu.VMEM)


def moved(tile, head, tiles, heads, dt, dh):
    return (lax.rem(tile + dt + tiles, tiles), lax.rem(head + dh + heads, heads))


def all_barrier(tile, head, tiles, heads):
    total = tiles * heads
    me = tile * heads + head
    barrier = pltpu.get_barrier_semaphore()

    def greet(k, carry):
        peer = lax.rem(me + k, total)
        pl.semaphore_signal(
            barrier, inc=1, device_id=(peer // heads, lax.rem(peer, heads)), device_id_type=MESH
        )
        return carry

    lax.fori_loop(1, total, greet, 0)
    pl.semaphore_wait(barrier, total - 1)


def stats_copy(stat_ref, slots_ref, send, recv, me, total, heads, k):
    peer = lax.rem(me + k, total)
    return pltpu.make_async_remote_copy(
        src_ref=stat_ref,
        dst_ref=slots_ref.at[k],
        send_sem=send.at[k],
        recv_sem=recv.at[k],
        device_id=(peer // heads, lax.rem(peer, heads)),
        device_id_type=MESH,
    )


def exchange_kernel(tiles, heads, plan, npay, *refs):
    stat_ref, pays = refs[0], refs[1 : 1 + npay]
    slots_ref, gots = refs[1 + npay], refs[2 + npay : 2 + npay + len(plan)]
    s_send, s_recv, p_send, p_recv = refs[2 + npay + len(plan) :]
    total = tiles * heads
    tile, head = lax.axis_index("tile"), lax.axis_index("head")
    me = tile * heads + head
    all_barrier(tile, head, tiles, heads)
    copies = []
    for i, (src, dt, dh) in enumerate(plan):
        copies.append(
            pltpu.make_async_remote_copy(
                src_ref=pays[src],
                dst_ref=gots[i],
                send_sem=p_send.at[i],
                recv_sem=p_recv.at[i],
                device_id=moved(tile, head, tiles, heads, dt, dh),
                device_id_type=MESH,
            )
        )
    one = functools.partial(stats_copy, stat_ref, slots_ref, s_send, s_recv, me, total, heads)

    def begin(k, carry):
        one(k).start()
        return carry

    def finish(k, carry):
        one(k).wait()
        return carry

    lax.fori_loop(1, total, begin, 0)
    for copy in copies:
        copy.start()
    slots_ref[0] = stat_ref[...]
    lax.fori_loop(1, total, finish, 0)
    for copy in copies:
        copy.wait()


def exchange(cid, stat, payloads, plan):
    tiles, heads = lax.axis_size("tile"), lax.axis_size("head")
    total = tiles * heads
    outs = [jax.ShapeDtypeStruct((total, 1, 128), jnp.float32)]
    outs += [jax.ShapeDtypeStruct(payloads[s].shape, payloads[s].dtype) for s, _, _ in plan]
    return pl.pallas_call(
        functools.partial(exchange_kernel, tiles, heads, plan, len(payloads)),
        out_shape=outs,
        in_specs=[VMEM] * (1 + len(payloads)),
        out_specs=[VMEM] * len(outs),
        scratch_shapes=[
            pltpu.SemaphoreType.DMA((total,)),
            pltpu.SemaphoreType.DMA((total,)),
            pltpu.SemaphoreType.DMA((len(plan),)),
            pltpu.SemaphoreType.DMA((len(plan),)),
        ],
        compiler_params=pltpu.CompilerParams(collective_id=cid, has_side_effects=True),
        name="exchange_%d" % cid,
    )(stat, *payloads)


def gather_kernel(tiles, heads, stat_ref, res_ref, slots_ref, kv_ref, q_ref, *sems):
    s_send, s_recv, z_send, z_recv, c_send, c_recv, q_send, q_recv = sems
    total = tiles * heads
    tile, head = lax.axis_index("tile"), lax.axis_index("head")
    me = tile * heads + head
    partner = (tile + 1 - 2 * lax.rem(tile, 2), head)
    all_barrier(tile, head, tiles, heads)
    one = functools.partial(stats_copy, stat_ref, slots_ref, s_send, s_recv, me, total, heads)

    def begin(k, carry):
        one(k).start()
        return carry

    def finish(k, carry):
        one(k).wait()
        return carry

    lax.fori_loop(1, total, begin, 0)

    def zcopy(k):
        return pltpu.make_async_remote_copy(
            src_ref=res_ref,
            dst_ref=kv_ref.at[0, k],
            send_sem=z_send.at[k],
            recv_sem=z_recv.at[k],
            device_id=(tile, lax.rem(head + k, heads)),
            device_id_type=MESH,
        )

    def ccopy(k):
        return pltpu.make_async_remote_copy(
            src_ref=res_ref if k == 0 else kv_ref.at[0, k],
            dst_ref=kv_ref.at[1, k],
            send_sem=c_send.at[k],
            recv_sem=c_recv.at[k],
            device_id=partner,
            device_id_type=MESH,
        )

    def qcopy(j):
        return pltpu.make_async_remote_copy(
            src_ref=res_ref,
            dst_ref=q_ref.at[j],
            send_sem=q_send.at[j],
            recv_sem=q_recv.at[j],
            device_id=(lax.rem(tile + 2 * j, tiles), head),
            device_id_type=MESH,
        )

    for k in range(1, heads):
        zcopy(k).start()
    for j in range(1, tiles // 2):
        qcopy(j).start()
    ccopy(0).start()
    kv_ref[0, 0] = res_ref[...]
    q_ref[0] = res_ref[...]
    slots_ref[0] = stat_ref[...]
    lax.fori_loop(1, total, finish, 0)
    for k in range(1, heads):
        zcopy(k).wait_recv()
        ccopy(k).start()
    for k in range(1, heads):
        zcopy(k).wait_send()
    for j in range(1, tiles // 2):
        qcopy(j).wait()
    for k in range(heads):
        ccopy(k).wait()


def gather(cid, stat, resid):
    tiles, heads = lax.axis_size("tile"), lax.axis_size("head")
    total = tiles * heads
    n, c = resid.shape
    dma = pltpu.SemaphoreType.DMA
    return pl.pallas_call(
        functools.partial(gather_kernel, tiles, heads),
        out_shape=[
            jax.ShapeDtypeStruct((total, 1, 128), jnp.float32),
            jax.ShapeDtypeStruct((2, heads, n, c), resid.dtype),
            jax.ShapeDtypeStruct((tiles // 2, n, c), resid.dtype),
        ],
        in_specs=[VMEM] * 2,
        out_specs=[VMEM] * 3,
        scratch_shapes=[dma((total,))] * 2
        + [dma((heads,))] * 4
        + [dma((tiles // 2,))] * 2,

        compiler_params=pltpu.CompilerParams(collective_id=cid, has_side_effects=True),
        name="gather_%d" % cid,
    )(stat, resid)


def scatter_kernel(tiles, heads, o_ref, l_ref, og_ref, lg_ref, o_send, o_recv, l_send, l_recv):
    tile, head = lax.axis_index("tile"), lax.axis_index("head")
    half = tiles // 2
    barrier = pltpu.get_barrier_semaphore()
    for j in range(1, half):
        pl.semaphore_signal(
            barrier,
            inc=1,
            device_id=(lax.rem(tile + 2 * j, tiles), head),
            device_id_type=MESH,
        )
    pl.semaphore_wait(barrier, half - 1)
    copies = []
    for src, dst, send, recv in ((l_ref, lg_ref, l_send, l_recv), (o_ref, og_ref, o_send, o_recv)):
        for j in range(1, half):
            copies.append(
                pltpu.make_async_remote_copy(
                    src_ref=src.at[j],
                    dst_ref=dst.at[j],
                    send_sem=send.at[j],
                    recv_sem=recv.at[j],
                    device_id=(lax.rem(tile + tiles - 2 * j, tiles), head),
                    device_id_type=MESH,
                )
            )
    for copy in copies:
        copy.start()
    og_ref[0] = o_ref[0]
    lg_ref[0] = l_ref[0]
    for copy in copies:
        copy.wait()


def scatter(cid, outs, lse):
    tiles, heads = lax.axis_size("tile"), lax.axis_size("head")
    dma = pltpu.SemaphoreType.DMA((tiles // 2,))
    return pl.pallas_call(
        functools.partial(scatter_kernel, tiles, heads),
        out_shape=[
            jax.ShapeDtypeStruct(outs.shape, outs.dtype),
            jax.ShapeDtypeStruct(lse.shape, lse.dtype),
        ],
        in_specs=[VMEM] * 2,
        out_specs=[VMEM] * 2,
        scratch_shapes=[dma] * 4,
        compiler_params=pltpu.CompilerParams(collective_id=cid, has_side_effects=True),
        name="scatter_%d" % cid,
    )(outs, lse)


def spread(per_group):
    return jnp.broadcast_to(per_group[:, None], (GROUPS, WIDTH)).reshape(C)


def local_stats(flat):
    count = flat.shape[0] * WIDTH
    mean = jnp.sum(jnp.sum(flat, axis=0).reshape(GROUPS, WIDTH), axis=1) / count
    deviation = flat - spread(mean)
    square = jnp.sum(jnp.sum(deviation * deviation, axis=0).reshape(GROUPS, WIDTH), axis=1)
    pad = jnp.zeros((128 - 2 * GROUPS,), jnp.float32)
    return jnp.concatenate([mean, square, pad]).reshape(1, 128)


def combined(slots, count, gain, shift):
    total = slots.shape[0]
    means, squares = slots[:, 0, :GROUPS], slots[:, 0, GROUPS : 2 * GROUPS]
    mean = jnp.sum(means, axis=0) / total
    gap = means - mean[None]
    variance = (jnp.sum(squares, axis=0) + count * jnp.sum(gap * gap, axis=0)) / (total * count)
    return spread(mean), spread(lax.rsqrt(variance + EPS)) * gain, shift


def normalize(values, norm):
    mean, scale, shift = norm
    return (values - mean) * scale + shift


def conv(act, weight):
    return lax.conv_general_dilated(
        act[None],
        weight,
        (1, 1),
        "VALID",
        dimension_numbers=("NHWC", "HWIO", "NHWC"),
        preferred_element_type=jnp.float32,
    )[0]


def inside(rows, cols, first_row, first_col, all_rows, all_cols):
    r = first_row + lax.broadcasted_iota(jnp.int32, (rows, cols, 1), 0)
    c = first_col + lax.broadcasted_iota(jnp.int32, (rows, cols, 1), 1)
    return (r >= 0) & (r < all_rows) & (c >= 0) & (c < all_cols)


def per_device(
    latent,
    norm1_gain,
    norm1_shift,
    conv1_weight,
    conv1_bias,
    norm2_gain,
    norm2_shift,
    conv2_weight,
    conv2_bias,
    norm3_gain,
    norm3_shift,
    query_weight,
    query_bias,
    key_weight,
    value_weight,
    value_bias,
    out_weight,
    out_bias,
):
    rows, cols, channels = latent.shape
    tiles, heads = lax.axis_size("tile"), lax.axis_size("head")
    tile, head = lax.axis_index("tile"), lax.axis_index("head")
    n = rows * cols
    count = n * WIDTH
    latent32 = latent.astype(jnp.float32)

    top, bottom = latent[:2], latent[rows - 2 :]
    west, east = latent[:, 0], latent[:, cols - 1]
    payloads = [top, bottom, west, east, west[:2], east[:2], west[rows - 2 :], east[rows - 2 :]]
    plan = (
        (1, 1, 0),
        (0, -1, 0),
        (3, 0, 1),
        (2, 0, -1),
        (7, 1, 1),
        (6, 1, -1),
        (5, -1, 1),
        (4, -1, -1),
    )
    slots, above, below, left, right, al, ar, bl, br = exchange(
        1, local_stats(latent32.reshape(n, C)), payloads, plan
    )
    lefts = jnp.concatenate([al, left, bl], axis=0)[:, None]
    rights = jnp.concatenate([ar, right, br], axis=0)[:, None]
    middle = jnp.concatenate([above, latent, below], axis=0)
    wide = jnp.concatenate([lefts, middle, rights], axis=1).astype(jnp.float32)
    first_row, first_col = tile * rows, head * cols
    all_rows, all_cols = rows * tiles, cols * heads
    act1 = jax.nn.silu(normalize(wide, combined(slots, count, norm1_gain, norm1_shift)))
    mask1 = inside(rows + 4, cols + 2, first_row - 2, first_col - 1, all_rows, all_cols)
    act1 = jnp.where(mask1, act1, 0.0).astype(jnp.bfloat16)
    hidden = conv(act1, conv1_weight) + conv1_bias

    slots, left, right = exchange(
        2,
        local_stats(hidden[1 : rows + 1].reshape(n, C)),
        [hidden[:, 0], hidden[:, cols - 1]],
        ((1, 0, 1), (0, 0, -1)),
    )
    wide = jnp.concatenate([left[:, None], hidden, right[:, None]], axis=1)
    act2 = jax.nn.silu(normalize(wide, combined(slots, count, norm2_gain, norm2_shift)))
    mask2 = inside(rows + 2, cols + 2, first_row - 1, first_col - 1, all_rows, all_cols)
    act2 = jnp.where(mask2, act2, 0.0).astype(jnp.bfloat16)
    resid = (latent32 + (conv(act2, conv2_weight) + conv2_bias)).astype(jnp.bfloat16)
    resid = resid.reshape(n, C)

    slots, kv_res, q_res = gather(3, local_stats(resid.astype(jnp.float32)), resid)
    norm3 = combined(slots, count, norm3_gain, norm3_shift)
    kv_in = normalize(kv_res.reshape(-1, C).astype(jnp.float32), norm3).astype(jnp.bfloat16)
    q_in = normalize(q_res.reshape(-1, C).astype(jnp.float32), norm3).astype(jnp.bfloat16)
    queries = (jnp.dot(q_in, query_weight, preferred_element_type=jnp.float32) + query_bias).astype(
        jnp.bfloat16
    )
    keys = jnp.dot(kv_in, key_weight, preferred_element_type=jnp.float32).astype(jnp.bfloat16)
    values = (
        jnp.dot(kv_in, value_weight, preferred_element_type=jnp.float32) + value_bias
    ).astype(jnp.bfloat16)
    softmax_scale = 1.0 / C**0.5

    def attend(block):
        scores = jnp.dot(block, keys.T, preferred_element_type=jnp.float32) * softmax_scale
        peak = jnp.max(scores, axis=1)
        expo = jnp.exp(scores - peak[:, None])
        total = jnp.sum(expo, axis=1)
        weighted = jnp.dot(expo.astype(jnp.bfloat16), values, preferred_element_type=jnp.float32)
        return (weighted / total[:, None]).astype(jnp.bfloat16), peak + jnp.log(total)

    half = tiles // 2
    blocks = 4 if half % 4 == 0 else half
    if half == blocks:
        part, lse = attend(queries)
    else:
        part, lse = lax.map(attend, queries.reshape(half // blocks, blocks * n, C))
    got, got_lse = scatter(4, part.reshape(half, n, C), lse.reshape(half, n // 128, 128))
    got_lse = got_lse.reshape(half, n)
    weight = jnp.exp(got_lse - jnp.max(got_lse, axis=0))
    weight = weight / jnp.sum(weight, axis=0)
    attended = jnp.sum(weight[:, :, None] * got.astype(jnp.float32), axis=0).astype(jnp.bfloat16)
    mixed = (
        resid.astype(jnp.float32)
        + jnp.dot(attended, out_weight, preferred_element_type=jnp.float32)
        + out_bias
    )
    return mixed.astype(jnp.bfloat16).reshape(rows, cols, C)


def solution(mesh):
    return jax.shard_map(
        per_device,
        mesh=mesh,
        in_specs=(P("tile", "head", None),) + (P(),) * 17,
        out_specs=P("tile", "head", None),
        check_vma=False,
    )
```

```python
import functools

import jax
import jax.numpy as jnp
from jax import lax
from jax.experimental import pallas as pl
from jax.experimental.pallas import tpu as pltpu
from jax.sharding import PartitionSpec as P

C = 512
GROUPS = 32
WIDTH = C // GROUPS
EPS = 1e-06
MESH = pl.DeviceIdType.MESH
VMEM = pl.BlockSpec(memory_space=pltpu.VMEM)


def moved(tile, head, tiles, heads, dt, dh):
    return (lax.rem(tile + dt + tiles, tiles), lax.rem(head + dh + heads, heads))


def all_barrier(tile, head, tiles, heads):
    total = tiles * heads
    me = tile * heads + head
    barrier = pltpu.get_barrier_semaphore()

    def greet(k, carry):
        peer = lax.rem(me + k, total)
        pl.semaphore_signal(
            barrier, inc=1, device_id=(peer // heads, lax.rem(peer, heads)), device_id_type=MESH
        )
        return carry

    lax.fori_loop(1, total, greet, 0)
    pl.semaphore_wait(barrier, total - 1)


def stats_copy(stat_ref, slots_ref, send, recv, me, total, heads, k):
    peer = lax.rem(me + k, total)
    return pltpu.make_async_remote_copy(
        src_ref=stat_ref,
        dst_ref=slots_ref.at[k],
        send_sem=send.at[k],
        recv_sem=recv.at[k],
        device_id=(peer // heads, lax.rem(peer, heads)),
        device_id_type=MESH,
    )


def exchange_kernel(tiles, heads, plan, npay, *refs):
    stat_ref, pays = refs[0], refs[1 : 1 + npay]
    slots_ref, gots = refs[1 + npay], refs[2 + npay : 2 + npay + len(plan)]
    s_send, s_recv, p_send, p_recv = refs[2 + npay + len(plan) :]
    total = tiles * heads
    tile, head = lax.axis_index("tile"), lax.axis_index("head")
    me = tile * heads + head
    all_barrier(tile, head, tiles, heads)
    copies = []
    for i, (src, dt, dh) in enumerate(plan):
        copies.append(
            pltpu.make_async_remote_copy(
                src_ref=pays[src],
                dst_ref=gots[i],
                send_sem=p_send.at[i],
                recv_sem=p_recv.at[i],
                device_id=moved(tile, head, tiles, heads, dt, dh),
                device_id_type=MESH,
            )
        )
    one = functools.partial(stats_copy, stat_ref, slots_ref, s_send, s_recv, me, total, heads)

    def begin(k, carry):
        one(k).start()
        return carry

    def finish(k, carry):
        one(k).wait()
        return carry

    lax.fori_loop(1, total, begin, 0)
    for copy in copies:
        copy.start()
    slots_ref[0] = stat_ref[...]
    lax.fori_loop(1, total, finish, 0)
    for copy in copies:
        copy.wait()


def exchange(cid, stat, payloads, plan):
    tiles, heads = lax.axis_size("tile"), lax.axis_size("head")
    total = tiles * heads
    outs = [jax.ShapeDtypeStruct((total, 1, 128), jnp.float32)]
    outs += [jax.ShapeDtypeStruct(payloads[s].shape, payloads[s].dtype) for s, _, _ in plan]
    return pl.pallas_call(
        functools.partial(exchange_kernel, tiles, heads, plan, len(payloads)),
        out_shape=outs,
        in_specs=[VMEM] * (1 + len(payloads)),
        out_specs=[VMEM] * len(outs),
        scratch_shapes=[
            pltpu.SemaphoreType.DMA((total,)),
            pltpu.SemaphoreType.DMA((total,)),
            pltpu.SemaphoreType.DMA((len(plan),)),
            pltpu.SemaphoreType.DMA((len(plan),)),
        ],
        compiler_params=pltpu.CompilerParams(collective_id=cid, has_side_effects=True),
        name="exchange_%d" % cid,
    )(stat, *payloads)


def gather_kernel(tiles, heads, stat_ref, res_ref, slots_ref, kv_ref, q_ref, *sems):
    s_send, s_recv, z_send, z_recv, c_send, c_recv, q_send, q_recv = sems
    total = tiles * heads
    tile, head = lax.axis_index("tile"), lax.axis_index("head")
    me = tile * heads + head
    partner = (tile + 1 - 2 * lax.rem(tile, 2), head)
    all_barrier(tile, head, tiles, heads)
    one = functools.partial(stats_copy, stat_ref, slots_ref, s_send, s_recv, me, total, heads)

    def begin(k, carry):
        one(k).start()
        return carry

    def finish(k, carry):
        one(k).wait()
        return carry

    lax.fori_loop(1, total, begin, 0)

    def zcopy(k):
        return pltpu.make_async_remote_copy(
            src_ref=res_ref,
            dst_ref=kv_ref.at[0, k],
            send_sem=z_send.at[k],
            recv_sem=z_recv.at[k],
            device_id=(tile, lax.rem(head + k, heads)),
            device_id_type=MESH,
        )

    def ccopy(k):
        return pltpu.make_async_remote_copy(
            src_ref=res_ref if k == 0 else kv_ref.at[0, k],
            dst_ref=kv_ref.at[1, k],
            send_sem=c_send.at[k],
            recv_sem=c_recv.at[k],
            device_id=partner,
            device_id_type=MESH,
        )

    def qcopy(j):
        return pltpu.make_async_remote_copy(
            src_ref=res_ref,
            dst_ref=q_ref.at[j],
            send_sem=q_send.at[j],
            recv_sem=q_recv.at[j],
            device_id=(lax.rem(tile + 2 * j, tiles), head),
            device_id_type=MESH,
        )

    for k in range(1, heads):
        zcopy(k).start()
    for j in range(1, tiles // 2):
        qcopy(j).start()
    ccopy(0).start()
    kv_ref[0, 0] = res_ref[...]
    q_ref[0] = res_ref[...]
    slots_ref[0] = stat_ref[...]
    lax.fori_loop(1, total, finish, 0)
    for k in range(1, heads):
        zcopy(k).wait_recv()
        ccopy(k).start()
    for k in range(1, heads):
        zcopy(k).wait_send()
    for j in range(1, tiles // 2):
        qcopy(j).wait()
    for k in range(heads):
        ccopy(k).wait()


def gather(cid, stat, resid):
    tiles, heads = lax.axis_size("tile"), lax.axis_size("head")
    total = tiles * heads
    n, c = resid.shape
    dma = pltpu.SemaphoreType.DMA
    return pl.pallas_call(
        functools.partial(gather_kernel, tiles, heads),
        out_shape=[
            jax.ShapeDtypeStruct((total, 1, 128), jnp.float32),
            jax.ShapeDtypeStruct((2, heads, n, c), resid.dtype),
            jax.ShapeDtypeStruct((tiles // 2, n, c), resid.dtype),
        ],
        in_specs=[VMEM] * 2,
        out_specs=[VMEM] * 3,
        scratch_shapes=[dma((total,))] * 2
        + [dma((heads,))] * 4
        + [dma((tiles // 2,))] * 2,

        compiler_params=pltpu.CompilerParams(collective_id=cid, has_side_effects=True),
        name="gather_%d" % cid,
    )(stat, resid)


def attend_kernel(
    tiles,
    heads,
    q_ref,
    k_ref,
    v_ref,
    res_ref,
    w_ref,
    b_ref,
    out_ref,
    o_scr,
    og_scr,
    l_scr,
    lg_scr,
    o_send,
    o_recv,
    l_send,
    l_recv,
):
    tile, head = lax.axis_index("tile"), lax.axis_index("head")
    half = tiles // 2
    n = res_ref.shape[0]
    barrier = pltpu.get_barrier_semaphore()
    for j in range(1, half):
        pl.semaphore_signal(
            barrier,
            inc=1,
            device_id=(lax.rem(tile + 2 * j, tiles), head),
            device_id_type=MESH,
        )
    pl.semaphore_wait(barrier, half - 1)
    softmax_scale = 1.0 / C**0.5

    def copies(j):
        owner = (lax.rem(tile + tiles - 2 * j, tiles), head)
        return [
            pltpu.make_async_remote_copy(
                src_ref=src.at[j],
                dst_ref=dst.at[j],
                send_sem=send.at[j],
                recv_sem=recv.at[j],
                device_id=owner,
                device_id_type=MESH,
            )
            for src, dst, send, recv in (
                (o_scr, og_scr, o_send, o_recv),
                (l_scr, lg_scr, l_send, l_recv),
            )
        ]

    def compute(j, o_to, l_to):
        scores = jnp.dot(q_ref[j], k_ref[...], preferred_element_type=jnp.float32) * softmax_scale
        peak = jnp.max(scores, axis=1, keepdims=True)
        expo = jnp.exp(scores - peak)
        total = jnp.sum(expo, axis=1, keepdims=True)
        weighted = jnp.dot(expo.astype(jnp.bfloat16), v_ref[...], preferred_element_type=jnp.float32)
        lse = jnp.broadcast_to(peak + jnp.log(total), (n, 128))
        l_to[j] = jnp.transpose(lse)[:8]
        o_to[j] = (weighted / total).astype(jnp.bfloat16)

    def step(j, carry):
        compute(j, o_scr, l_scr)
        for copy in copies(j):
            copy.start()
        return carry

    lax.fori_loop(1, half, step, 0)
    compute(0, og_scr, lg_scr)
    for j in range(1, half):
        for copy in copies(j):
            copy.wait()
    peak = lg_scr[0]
    for j in range(1, half):
        peak = jnp.maximum(peak, lg_scr[j])
    weights = [jnp.exp(lg_scr[j] - peak) for j in range(half)]
    total = weights[0]
    for j in range(1, half):
        total = total + weights[j]
    mixed = jnp.zeros((n, C), jnp.float32)
    for j in range(half):
        column = jnp.transpose(jnp.broadcast_to((weights[j] / total)[:1], (128, n)))[:, :1]
        mixed = mixed + column * og_scr[j].astype(jnp.float32)
    out = jnp.dot(mixed.astype(jnp.bfloat16), w_ref[...], preferred_element_type=jnp.float32)
    out_ref[...] = (res_ref[...].astype(jnp.float32) + out + b_ref[...]).astype(jnp.bfloat16)


def attend(cid, queries, keys, values, resid, weight, bias):
    tiles, heads = lax.axis_size("tile"), lax.axis_size("head")
    half = tiles // 2
    n = resid.shape[0]
    dma = pltpu.SemaphoreType.DMA((half,))
    return pl.pallas_call(
        functools.partial(attend_kernel, tiles, heads),
        out_shape=jax.ShapeDtypeStruct(resid.shape, resid.dtype),
        in_specs=[VMEM] * 6,
        out_specs=VMEM,
        scratch_shapes=[pltpu.VMEM((half, n, C), jnp.bfloat16)] * 2
        + [pltpu.VMEM((half, 8, n), jnp.float32)] * 2
        + [dma] * 4,
        compiler_params=pltpu.CompilerParams(collective_id=cid, has_side_effects=True),
        name="attend_%d" % cid,
    )(queries, keys, values, resid, weight, bias)


def conv_kernel(act_ref, w_ref, b_ref, out_ref, lhs):
    rows, cols = act_ref.shape[0] - 2, act_ref.shape[1] - 2

    @pl.when(pl.program_id(0) == 0)
    def unfold():
        for dj in range(3):
            moved_cols = act_ref[:, dj : dj + cols, :]
            for di in range(3):
                tap = 3 * di + dj
                lhs[:, tap * C : (tap + 1) * C] = moved_cols[di : di + rows].reshape(rows * cols, C)

    out_ref[...] = (
        jnp.dot(lhs[...], w_ref[...], preferred_element_type=jnp.float32) + b_ref[...]
    )


def conv(act, weight, bias):
    rows, cols = act.shape[0] - 2, act.shape[1] - 2
    part = C // 2
    out = pl.pallas_call(
        conv_kernel,
        grid=(C // part,),
        out_shape=jax.ShapeDtypeStruct((rows * cols, C), jnp.float32),
        in_specs=[
            pl.BlockSpec(act.shape, lambda i: (0, 0, 0)),
            pl.BlockSpec((9 * C, part), lambda i: (0, i)),
            pl.BlockSpec((1, part), lambda i: (0, i)),
        ],
        out_specs=pl.BlockSpec((rows * cols, part), lambda i: (0, i)),
        scratch_shapes=[pltpu.VMEM((rows * cols, 9 * C), jnp.bfloat16)],
        cost_estimate=pl.CostEstimate(
            flops=2 * rows * cols * 9 * C * C, bytes_accessed=18 * C * C, transcendentals=0
        ),
        name="conv_%d" % rows,
    )(act, weight.reshape(9 * C, C), bias.reshape(1, C))
    return out.reshape(rows, cols, C)


def spread(per_group):
    return jnp.broadcast_to(per_group[:, None], (GROUPS, WIDTH)).reshape(C)


def local_stats(flat):
    count = flat.shape[0] * WIDTH
    mean = jnp.sum(jnp.sum(flat, axis=0).reshape(GROUPS, WIDTH), axis=1) / count
    deviation = flat - spread(mean)
    square = jnp.sum(jnp.sum(deviation * deviation, axis=0).reshape(GROUPS, WIDTH), axis=1)
    pad = jnp.zeros((128 - 2 * GROUPS,), jnp.float32)
    return jnp.concatenate([mean, square, pad]).reshape(1, 128)


def combined(slots, count, gain, shift):
    total = slots.shape[0]
    means, squares = slots[:, 0, :GROUPS], slots[:, 0, GROUPS : 2 * GROUPS]
    mean = jnp.sum(means, axis=0) / total
    gap = means - mean[None]
    variance = (jnp.sum(squares, axis=0) + count * jnp.sum(gap * gap, axis=0)) / (total * count)
    return spread(mean), spread(lax.rsqrt(variance + EPS)) * gain, shift


def normalize(values, norm):
    mean, scale, shift = norm
    return (values - mean) * scale + shift


def inside(rows, cols, first_row, first_col, all_rows, all_cols):
    r = first_row + lax.broadcasted_iota(jnp.int32, (rows, cols, 1), 0)
    c = first_col + lax.broadcasted_iota(jnp.int32, (rows, cols, 1), 1)
    return (r >= 0) & (r < all_rows) & (c >= 0) & (c < all_cols)


def per_device(
    latent,
    norm1_gain,
    norm1_shift,
    conv1_weight,
    conv1_bias,
    norm2_gain,
    norm2_shift,
    conv2_weight,
    conv2_bias,
    norm3_gain,
    norm3_shift,
    query_weight,
    query_bias,
    key_weight,
    value_weight,
    value_bias,
    out_weight,
    out_bias,
):
    rows, cols, channels = latent.shape
    tiles, heads = lax.axis_size("tile"), lax.axis_size("head")
    tile, head = lax.axis_index("tile"), lax.axis_index("head")
    n = rows * cols
    count = n * WIDTH
    latent32 = latent.astype(jnp.float32)

    top, bottom = latent[:2], latent[rows - 2 :]
    west, east = latent[:, 0], latent[:, cols - 1]
    payloads = [top, bottom, west, east, west[:2], east[:2], west[rows - 2 :], east[rows - 2 :]]
    plan = (
        (1, 1, 0),
        (0, -1, 0),
        (3, 0, 1),
        (2, 0, -1),
        (7, 1, 1),
        (6, 1, -1),
        (5, -1, 1),
        (4, -1, -1),
    )
    slots, above, below, left, right, al, ar, bl, br = exchange(
        1, local_stats(latent32.reshape(n, C)), payloads, plan
    )
    lefts = jnp.concatenate([al, left, bl], axis=0)[:, None]
    rights = jnp.concatenate([ar, right, br], axis=0)[:, None]
    middle = jnp.concatenate([above, latent, below], axis=0)
    wide = jnp.concatenate([lefts, middle, rights], axis=1).astype(jnp.float32)
    first_row, first_col = tile * rows, head * cols
    all_rows, all_cols = rows * tiles, cols * heads
    act1 = jax.nn.silu(normalize(wide, combined(slots, count, norm1_gain, norm1_shift)))
    mask1 = inside(rows + 4, cols + 2, first_row - 2, first_col - 1, all_rows, all_cols)
    act1 = jnp.where(mask1, act1, 0.0).astype(jnp.bfloat16)
    hidden = conv(act1, conv1_weight, conv1_bias)

    slots, left, right = exchange(
        2,
        local_stats(hidden[1 : rows + 1].reshape(n, C)),
        [hidden[:, 0], hidden[:, cols - 1]],
        ((1, 0, 1), (0, 0, -1)),
    )
    wide = jnp.concatenate([left[:, None], hidden, right[:, None]], axis=1)
    act2 = jax.nn.silu(normalize(wide, combined(slots, count, norm2_gain, norm2_shift)))
    mask2 = inside(rows + 2, cols + 2, first_row - 1, first_col - 1, all_rows, all_cols)
    act2 = jnp.where(mask2, act2, 0.0).astype(jnp.bfloat16)
    resid = (latent32 + conv(act2, conv2_weight, conv2_bias)).astype(jnp.bfloat16)
    resid = resid.reshape(n, C)

    slots, kv_res, q_res = gather(3, local_stats(resid.astype(jnp.float32)), resid)
    norm3 = combined(slots, count, norm3_gain, norm3_shift)
    kv_in = normalize(kv_res.reshape(-1, C).astype(jnp.float32), norm3).astype(jnp.bfloat16)
    q_in = normalize(q_res.reshape(-1, C).astype(jnp.float32), norm3).astype(jnp.bfloat16)
    queries = (jnp.dot(q_in, query_weight, preferred_element_type=jnp.float32) + query_bias).astype(
        jnp.bfloat16
    )
    keys = lax.dot_general(
        key_weight, kv_in, (((0,), (1,)), ((), ())), preferred_element_type=jnp.float32
    ).astype(jnp.bfloat16)
    values = (
        jnp.dot(kv_in, value_weight, preferred_element_type=jnp.float32) + value_bias
    ).astype(jnp.bfloat16)
    mixed = attend(
        4, queries.reshape(-1, n, C), keys, values, resid, out_weight, out_bias.reshape(1, C)
    )
    return mixed.reshape(rows, cols, C)


def solution(mesh):
    return jax.shard_map(
        per_device,
        mesh=mesh,
        in_specs=(P("tile", "head", None),) + (P(),) * 17,
        out_specs=P("tile", "head", None),
        check_vma=False,
    )
```

```python
import functools

import jax
import jax.numpy as jnp
from jax import lax
from jax.experimental import pallas as pl
from jax.experimental.pallas import tpu as pltpu
from jax.sharding import PartitionSpec as P

C = 512
GROUPS = 32
WIDTH = C // GROUPS
EPS = 1e-06
MESH = pl.DeviceIdType.MESH
VMEM = pl.BlockSpec(memory_space=pltpu.VMEM)


def moved(tile, head, tiles, heads, dt, dh):
    return (lax.rem(tile + dt + tiles, tiles), lax.rem(head + dh + heads, heads))


def greet_all(tile, head, tiles, heads):
    total = tiles * heads
    me = tile * heads + head
    barrier = pltpu.get_barrier_semaphore()

    def greet(k, carry):
        peer = lax.rem(me + k, total)
        pl.semaphore_signal(
            barrier, inc=1, device_id=(peer // heads, lax.rem(peer, heads)), device_id_type=MESH
        )
        return carry

    lax.fori_loop(1, total, greet, 0)


def group_dot(row, onehot, axis):
    return lax.dot_general(
        jnp.broadcast_to(row, (8, row.shape[1])),
        onehot,
        (((1,), (axis,)), ((), ())),
        precision=lax.Precision.HIGHEST,
        preferred_element_type=jnp.float32,
    )[:1]


def membership():
    channel = lax.broadcasted_iota(jnp.int32, (C, 128), 0)
    first = lax.broadcasted_iota(jnp.int32, (C, 128), 1) * WIDTH
    return jnp.where((channel >= first) & (channel < first + WIDTH), 1.0, 0.0)


def store_stats(values, stat_ref):
    onehot = membership()
    values = values.astype(jnp.float32)
    sums = group_dot(jnp.sum(values, axis=0, keepdims=True), onehot, 0)
    mean = sums / (values.shape[0] * WIDTH)
    deviation = values - group_dot(mean, onehot, 1)
    stat_ref[0:1] = mean
    stat_ref[1:2] = group_dot(jnp.sum(deviation * deviation, axis=0, keepdims=True), onehot, 0)


def store_norm(slots_ref, norm_ref, count):
    onehot = membership()
    slots = slots_ref[...]
    total = slots.shape[0]
    sums = jnp.sum(slots, axis=0)
    mean = sums[0:1] / total
    gap = slots[:, 0:1, :] - mean[None]
    variance = (sums[1:2] + count * jnp.sum(gap * gap, axis=0)) / (total * count)
    norm_ref[0:1] = group_dot(mean, onehot, 1)
    norm_ref[1:2] = group_dot(lax.rsqrt(variance + EPS), onehot, 1)


def stats_copy(stat_ref, slots_ref, send, recv, me, total, heads, k):
    peer = lax.rem(me + k, total)
    return pltpu.make_async_remote_copy(
        src_ref=stat_ref,
        dst_ref=slots_ref.at[k],
        send_sem=send.at[k],
        recv_sem=recv.at[k],
        device_id=(peer // heads, lax.rem(peer, heads)),
        device_id_type=MESH,
    )


def exchange_kernel(tiles, heads, plan, npay, *refs):
    values_ref, pays = refs[0], refs[1 : 1 + npay]
    norm_ref, gots = refs[1 + npay], refs[2 + npay : 2 + npay + len(plan)]
    stat_ref, slots_ref, s_send, s_recv, p_send, p_recv = refs[2 + npay + len(plan) :]
    total = tiles * heads
    tile, head = lax.axis_index("tile"), lax.axis_index("head")
    me = tile * heads + head
    greet_all(tile, head, tiles, heads)
    store_stats(values_ref[...], stat_ref)
    slots_ref[0] = stat_ref[...]
    pl.semaphore_wait(pltpu.get_barrier_semaphore(), total - 1)
    copies = []
    for i, (src, dt, dh) in enumerate(plan):
        copies.append(
            pltpu.make_async_remote_copy(
                src_ref=pays[src],
                dst_ref=gots[i],
                send_sem=p_send.at[i],
                recv_sem=p_recv.at[i],
                device_id=moved(tile, head, tiles, heads, dt, dh),
                device_id_type=MESH,
            )
        )
    one = functools.partial(stats_copy, stat_ref, slots_ref, s_send, s_recv, me, total, heads)

    def begin(k, carry):
        one(k).start()
        return carry

    def finish(k, carry):
        one(k).wait()
        return carry

    lax.fori_loop(1, total, begin, 0)
    for copy in copies:
        copy.start()
    lax.fori_loop(1, total, finish, 0)
    store_norm(slots_ref, norm_ref, values_ref.shape[0] * WIDTH)
    for copy in copies:
        copy.wait()


def exchange(cid, stat, payloads, plan):
    tiles, heads = lax.axis_size("tile"), lax.axis_size("head")
    total = tiles * heads
    outs = [jax.ShapeDtypeStruct((2, C), jnp.float32)]
    outs += [jax.ShapeDtypeStruct(payloads[s].shape, payloads[s].dtype) for s, _, _ in plan]
    return pl.pallas_call(
        functools.partial(exchange_kernel, tiles, heads, plan, len(payloads)),
        out_shape=outs,
        in_specs=[VMEM] * (1 + len(payloads)),
        out_specs=[VMEM] * len(outs),
        scratch_shapes=[
            pltpu.VMEM((2, 128), jnp.float32),
            pltpu.VMEM((total, 2, 128), jnp.float32),
            pltpu.SemaphoreType.DMA((total,)),
            pltpu.SemaphoreType.DMA((total,)),
            pltpu.SemaphoreType.DMA((len(plan),)),
            pltpu.SemaphoreType.DMA((len(plan),)),
        ],
        compiler_params=pltpu.CompilerParams(collective_id=cid, has_side_effects=True),
        name="exchange_%d" % cid,
    )(stat, *payloads)


def gather_kernel(
    tiles, heads, res_ref, norm_ref, kv_ref, q_ref, stat_ref, slots_ref, *sems
):
    s_send, s_recv, z_send, z_recv, c_send, c_recv, q_send, q_recv = sems
    total = tiles * heads
    tile, head = lax.axis_index("tile"), lax.axis_index("head")
    me = tile * heads + head
    partner = (tile + 1 - 2 * lax.rem(tile, 2), head)
    greet_all(tile, head, tiles, heads)
    store_stats(res_ref[...], stat_ref)
    slots_ref[0] = stat_ref[...]
    pl.semaphore_wait(pltpu.get_barrier_semaphore(), total - 1)
    one = functools.partial(stats_copy, stat_ref, slots_ref, s_send, s_recv, me, total, heads)

    def begin(k, carry):
        one(k).start()
        return carry

    def finish(k, carry):
        one(k).wait()
        return carry

    lax.fori_loop(1, total, begin, 0)

    def zcopy(k):
        return pltpu.make_async_remote_copy(
            src_ref=res_ref,
            dst_ref=kv_ref.at[0, k],
            send_sem=z_send.at[k],
            recv_sem=z_recv.at[k],
            device_id=(tile, lax.rem(head + k, heads)),
            device_id_type=MESH,
        )

    def ccopy(k):
        return pltpu.make_async_remote_copy(
            src_ref=res_ref if k == 0 else kv_ref.at[0, k],
            dst_ref=kv_ref.at[1, k],
            send_sem=c_send.at[k],
            recv_sem=c_recv.at[k],
            device_id=partner,
            device_id_type=MESH,
        )

    def qcopy(j):
        return pltpu.make_async_remote_copy(
            src_ref=res_ref,
            dst_ref=q_ref.at[j],
            send_sem=q_send.at[j],
            recv_sem=q_recv.at[j],
            device_id=(lax.rem(tile + 2 * j, tiles), head),
            device_id_type=MESH,
        )

    for k in range(1, heads):
        zcopy(k).start()
    for j in range(1, tiles // 2):
        qcopy(j).start()
    ccopy(0).start()
    kv_ref[0, 0] = res_ref[...]
    q_ref[0] = res_ref[...]
    lax.fori_loop(1, total, finish, 0)
    store_norm(slots_ref, norm_ref, res_ref.shape[0] * WIDTH)
    for k in range(1, heads):
        zcopy(k).wait_recv()
        ccopy(k).start()
    for k in range(1, heads):
        zcopy(k).wait_send()
    for j in range(1, tiles // 2):
        qcopy(j).wait()
    for k in range(heads):
        ccopy(k).wait()


def gather(cid, resid):
    tiles, heads = lax.axis_size("tile"), lax.axis_size("head")
    total = tiles * heads
    n, c = resid.shape
    dma = pltpu.SemaphoreType.DMA
    return pl.pallas_call(
        functools.partial(gather_kernel, tiles, heads),
        out_shape=[
            jax.ShapeDtypeStruct((2, C), jnp.float32),
            jax.ShapeDtypeStruct((2, heads, n, c), resid.dtype),
            jax.ShapeDtypeStruct((tiles // 2, n, c), resid.dtype),
        ],
        in_specs=[VMEM],
        out_specs=[VMEM] * 3,
        scratch_shapes=[
            pltpu.VMEM((2, 128), jnp.float32),
            pltpu.VMEM((total, 2, 128), jnp.float32),
        ]
        + [dma((total,))] * 2
        + [dma((heads,))] * 4
        + [dma((tiles // 2,))] * 2,

        compiler_params=pltpu.CompilerParams(collective_id=cid, has_side_effects=True),
        name="gather_%d" % cid,
    )(resid)


def attend_kernel(
    tiles,
    heads,
    q_ref,
    k_ref,
    v_ref,
    res_ref,
    w_ref,
    b_ref,
    out_ref,
    o_scr,
    og_scr,
    l_scr,
    lg_scr,
    o_send,
    o_recv,
    l_send,
    l_recv,
):
    tile, head = lax.axis_index("tile"), lax.axis_index("head")
    half = tiles // 2
    n = res_ref.shape[0]
    barrier = pltpu.get_barrier_semaphore()
    for j in range(1, half):
        pl.semaphore_signal(
            barrier,
            inc=1,
            device_id=(lax.rem(tile + 2 * j, tiles), head),
            device_id_type=MESH,
        )
    pl.semaphore_wait(barrier, half - 1)
    softmax_scale = 1.0 / C**0.5

    def copies(j):
        owner = (lax.rem(tile + tiles - 2 * j, tiles), head)
        return [
            pltpu.make_async_remote_copy(
                src_ref=src.at[j],
                dst_ref=dst.at[j],
                send_sem=send.at[j],
                recv_sem=recv.at[j],
                device_id=owner,
                device_id_type=MESH,
            )
            for src, dst, send, recv in (
                (o_scr, og_scr, o_send, o_recv),
                (l_scr, lg_scr, l_send, l_recv),
            )
        ]

    def compute(j, o_to, l_to):
        scores = jnp.dot(q_ref[j], k_ref[...], preferred_element_type=jnp.float32) * softmax_scale
        peak = jnp.max(scores, axis=1, keepdims=True)
        expo = jnp.exp(scores - peak)
        total = jnp.sum(expo, axis=1, keepdims=True)
        weighted = jnp.dot(expo.astype(jnp.bfloat16), v_ref[...], preferred_element_type=jnp.float32)
        lse = jnp.broadcast_to(peak + jnp.log(total), (n, 128))
        l_to[j] = jnp.transpose(lse)[:8]
        o_to[j] = (weighted / total).astype(jnp.bfloat16)

    def step(j, carry):
        compute(j, o_scr, l_scr)
        for copy in copies(j):
            copy.start()
        return carry

    lax.fori_loop(1, half, step, 0)
    compute(0, og_scr, lg_scr)
    for j in range(1, half):
        for copy in copies(j):
            copy.wait()
    peak = lg_scr[0]
    for j in range(1, half):
        peak = jnp.maximum(peak, lg_scr[j])
    weights = [jnp.exp(lg_scr[j] - peak) for j in range(half)]
    total = weights[0]
    for j in range(1, half):
        total = total + weights[j]
    mixed = jnp.zeros((n, C), jnp.float32)
    for j in range(half):
        column = jnp.transpose(jnp.broadcast_to((weights[j] / total)[:1], (128, n)))[:, :1]
        mixed = mixed + column * og_scr[j].astype(jnp.float32)
    out = jnp.dot(mixed.astype(jnp.bfloat16), w_ref[...], preferred_element_type=jnp.float32)
    out_ref[...] = (res_ref[...].astype(jnp.float32) + out + b_ref[...]).astype(jnp.bfloat16)


def attend(cid, queries, keys, values, resid, weight, bias):
    tiles, heads = lax.axis_size("tile"), lax.axis_size("head")
    half = tiles // 2
    n = resid.shape[0]
    dma = pltpu.SemaphoreType.DMA((half,))
    return pl.pallas_call(
        functools.partial(attend_kernel, tiles, heads),
        out_shape=jax.ShapeDtypeStruct(resid.shape, resid.dtype),
        in_specs=[VMEM] * 6,
        out_specs=VMEM,
        scratch_shapes=[pltpu.VMEM((half, n, C), jnp.bfloat16)] * 2
        + [pltpu.VMEM((half, 8, n), jnp.float32)] * 2
        + [dma] * 4,
        compiler_params=pltpu.CompilerParams(collective_id=cid, has_side_effects=True),
        name="attend_%d" % cid,
    )(queries, keys, values, resid, weight, bias)


def conv_kernel(act_ref, w_ref, b_ref, out_ref, lhs):
    rows, cols = act_ref.shape[0] - 2, act_ref.shape[1] - 2

    @pl.when(pl.program_id(0) == 0)
    def unfold():
        for dj in range(3):
            moved_cols = act_ref[:, dj : dj + cols, :]
            for di in range(3):
                tap = 3 * di + dj
                lhs[:, tap * C : (tap + 1) * C] = moved_cols[di : di + rows].reshape(rows * cols, C)

    out_ref[...] = (
        jnp.dot(lhs[...], w_ref[...], preferred_element_type=jnp.float32) + b_ref[...]
    )


def conv(act, weight, bias):
    rows, cols = act.shape[0] - 2, act.shape[1] - 2
    part = C // 2
    out = pl.pallas_call(
        conv_kernel,
        grid=(C // part,),
        out_shape=jax.ShapeDtypeStruct((rows * cols, C), jnp.float32),
        in_specs=[
            pl.BlockSpec(act.shape, lambda i: (0, 0, 0)),
            pl.BlockSpec((9 * C, part), lambda i: (0, i)),
            pl.BlockSpec((1, part), lambda i: (0, i)),
        ],
        out_specs=pl.BlockSpec((rows * cols, part), lambda i: (0, i)),
        scratch_shapes=[pltpu.VMEM((rows * cols, 9 * C), jnp.bfloat16)],
        cost_estimate=pl.CostEstimate(
            flops=2 * rows * cols * 9 * C * C, bytes_accessed=18 * C * C, transcendentals=0
        ),
        name="conv_%d" % rows,
    )(act, weight.reshape(9 * C, C), bias.reshape(1, C))
    return out.reshape(rows, cols, C)


def combined(norm, gain, shift):
    return norm[0], norm[1] * gain, shift


def normalize(values, norm):
    mean, scale, shift = norm
    return (values - mean) * scale + shift


def inside(rows, cols, first_row, first_col, all_rows, all_cols):
    r = first_row + lax.broadcasted_iota(jnp.int32, (rows, cols, 1), 0)
    c = first_col + lax.broadcasted_iota(jnp.int32, (rows, cols, 1), 1)
    return (r >= 0) & (r < all_rows) & (c >= 0) & (c < all_cols)


def per_device(
    latent,
    norm1_gain,
    norm1_shift,
    conv1_weight,
    conv1_bias,
    norm2_gain,
    norm2_shift,
    conv2_weight,
    conv2_bias,
    norm3_gain,
    norm3_shift,
    query_weight,
    query_bias,
    key_weight,
    value_weight,
    value_bias,
    out_weight,
    out_bias,
):
    rows, cols, channels = latent.shape
    tiles, heads = lax.axis_size("tile"), lax.axis_size("head")
    tile, head = lax.axis_index("tile"), lax.axis_index("head")
    n = rows * cols
    latent32 = latent.astype(jnp.float32)

    top, bottom = latent[:2], latent[rows - 2 :]
    west, east = latent[:, 0], latent[:, cols - 1]
    payloads = [top, bottom, west, east, west[:2], east[:2], west[rows - 2 :], east[rows - 2 :]]
    plan = (
        (1, 1, 0),
        (0, -1, 0),
        (3, 0, 1),
        (2, 0, -1),
        (7, 1, 1),
        (6, 1, -1),
        (5, -1, 1),
        (4, -1, -1),
    )
    slots, above, below, left, right, al, ar, bl, br = exchange(
        1, latent.reshape(n, C), payloads, plan
    )
    lefts = jnp.concatenate([al, left, bl], axis=0)[:, None]
    rights = jnp.concatenate([ar, right, br], axis=0)[:, None]
    middle = jnp.concatenate([above, latent, below], axis=0)
    wide = jnp.concatenate([lefts, middle, rights], axis=1).astype(jnp.float32)
    first_row, first_col = tile * rows, head * cols
    all_rows, all_cols = rows * tiles, cols * heads
    act1 = jax.nn.silu(normalize(wide, combined(slots, norm1_gain, norm1_shift)))
    mask1 = inside(rows + 4, cols + 2, first_row - 2, first_col - 1, all_rows, all_cols)
    act1 = jnp.where(mask1, act1, 0.0).astype(jnp.bfloat16)
    hidden = conv(act1, conv1_weight, conv1_bias)

    slots, left, right = exchange(
        2,
        hidden[1 : rows + 1].reshape(n, C),
        [hidden[:, 0], hidden[:, cols - 1]],
        ((1, 0, 1), (0, 0, -1)),
    )
    wide = jnp.concatenate([left[:, None], hidden, right[:, None]], axis=1)
    act2 = jax.nn.silu(normalize(wide, combined(slots, norm2_gain, norm2_shift)))
    mask2 = inside(rows + 2, cols + 2, first_row - 1, first_col - 1, all_rows, all_cols)
    act2 = jnp.where(mask2, act2, 0.0).astype(jnp.bfloat16)
    resid = (latent32 + conv(act2, conv2_weight, conv2_bias)).astype(jnp.bfloat16)
    resid = resid.reshape(n, C)

    slots, kv_res, q_res = gather(3, resid)
    norm3 = combined(slots, norm3_gain, norm3_shift)
    kv_in = normalize(kv_res.reshape(-1, C).astype(jnp.float32), norm3).astype(jnp.bfloat16)
    q_in = normalize(q_res.reshape(-1, C).astype(jnp.float32), norm3).astype(jnp.bfloat16)
    queries = (jnp.dot(q_in, query_weight, preferred_element_type=jnp.float32) + query_bias).astype(
        jnp.bfloat16
    )
    keys = lax.dot_general(
        key_weight, kv_in, (((0,), (1,)), ((), ())), preferred_element_type=jnp.float32
    ).astype(jnp.bfloat16)
    values = (
        jnp.dot(kv_in, value_weight, preferred_element_type=jnp.float32) + value_bias
    ).astype(jnp.bfloat16)
    mixed = attend(
        4, queries.reshape(-1, n, C), keys, values, resid, out_weight, out_bias.reshape(1, C)
    )
    return mixed.reshape(rows, cols, C)


def solution(mesh):
    return jax.shard_map(
        per_device,
        mesh=mesh,
        in_specs=(P("tile", "head", None),) + (P(),) * 17,
        out_specs=P("tile", "head", None),
        check_vma=False,
    )
```
